256 devices in a mesh: samp: 4 (over z_hi, core), snp: 64 (over y, z_lo, x).
Axes of the slice: x: 4, y: 4, z: 8 (z_hi: 2, z_lo: 4; z = z_hi * 4 + z_lo), core: 2. Of those that a mesh axis runs over, the one named last changes fastest.
Arguments:
- genotypes: float32 [4096, 65536], P('samp', 'snp'), may hold values from -1 to 2, as said below
Outputs:
- band_r: float32 [65536, 4096], P('snp', 'samp')
The draws below stay inside these ranges and needn't reach their ends.
Inputs may be any that keep to these rules, and one draw needn't show every extreme that they name: `genotypes`: -1 marks a missing dosage; every other value lies between 0 and 2. Every eighth sample (samples 0, 8, 16, ...) has no missing dosage, and over those samples each SNP's dosages run through 0, 1, 2 cyclically from a SNP's own starting value.
All inputs are finite; a program needn't handle non-finite values.
Results may differ from the reference program's by a relative error of at most 0.006.
Values may be sent and summed in bfloat16 or wider, within the bound.
A program may use at most 64 MiB of HBM per device.

```python
import jax
import jax.numpy as jnp
from jax import lax

TILE = 512
BAND = 4096
NSAMP = 4096
NSNP = 65536


def draw_genotypes(key, part):
    window = 32
    key_bits = jax.random.fold_in(key, 11)
    key_offset = jax.random.fold_in(key, 12)
    key_cycle = jax.random.fold_in(key, 13)
    key_missing = jax.random.fold_in(key, 14)
    key_jitter = jax.random.fold_in(key, 15)
    bits = jax.random.randint(key_bits, (NSAMP, NSNP + window), 0, 2, dtype=jnp.int32)
    running = jnp.cumsum(bits, axis=1)
    window_sum = running[:, window:] - running[:, :-window]
    offset = jax.random.randint(key_offset, (NSNP,), -4, 5, dtype=jnp.int32)
    sample_row = jnp.arange(NSAMP, dtype=jnp.int32)
    drift = 6 * sample_row // NSAMP
    level = (window_sum + offset[None, :] + drift[:, None]).astype(jnp.float32)
    jitter = jax.random.uniform(key_jitter, (NSAMP, NSNP), jnp.float32, 0.0, 1.0)
    temper = 2.0
    dosage = 2.0 * jax.nn.sigmoid((level + jitter - 19.0) / temper)
    cycle_start = jax.random.randint(key_cycle, (NSNP,), 0, 3, dtype=jnp.int32)
    anchor = (sample_row % 8 == 0)[:, None]
    cycled = ((sample_row[:, None] // 8 + cycle_start[None, :]) % 3).astype(jnp.float32)
    dosage = jnp.where(anchor, cycled, dosage)
    percent = 3 + 9 * sample_row // NSAMP
    missing_roll = jax.random.randint(key_missing, (NSAMP, NSNP), 0, 100, dtype=jnp.int32)
    missing = (missing_roll < percent[:, None]) & jnp.logical_not(anchor)
    return jnp.where(missing, -1.0, dosage).astype(jnp.float32)


def setup_inputs(seed: int = 0) -> dict:
    splits = jax.random.split(jax.random.key(seed), 2)
    genotypes = draw_genotypes(jax.random.fold_in(splits[1], 71), 0)
    return dict(genotypes=genotypes)


EPS = 1e-05

def reference(genotypes):
    present = (genotypes >= 0).astype(jnp.float32)
    dosage = genotypes.astype(jnp.float32) * present
    counted = lax.optimization_barrier(jnp.sum(present, axis=0))
    summed = lax.optimization_barrier(jnp.sum(dosage, axis=0))
    squared = lax.optimization_barrier(jnp.sum(dosage * dosage, axis=0))
    average = summed / counted
    spread = squared / counted - average * average
    scaled = (present * (dosage - average) * lax.rsqrt(spread + EPS)).astype(jnp.bfloat16)
    col_norms = counted * spread / (spread + EPS)
    total_snps = genotypes.shape[1]
    padded = jnp.concatenate([scaled, jnp.zeros((scaled.shape[0], BAND), scaled.dtype)], axis=1)
    padded_norms = jnp.concatenate([col_norms, jnp.ones((BAND,), jnp.float32)])

    def band_tile(tile_pos):
        start = (tile_pos * TILE).astype(jnp.int32)
        row_block = lax.dynamic_slice_in_dim(scaled, start, TILE, 1)
        col_block = lax.dynamic_slice_in_dim(padded, start, BAND, 1)
        products = lax.dot_general(row_block, col_block, (((0,), (0,)), ((), ())), preferred_element_type=jnp.float32)
        row_norm = lax.dynamic_slice_in_dim(col_norms, start, TILE, 0)
        col_norm = lax.dynamic_slice_in_dim(padded_norms, start, BAND, 0)
        return products / jnp.sqrt(row_norm[:, None] * col_norm[None, :])
    tiles = lax.map(band_tile, jnp.arange(total_snps // TILE, dtype=jnp.int32))
    return tiles.reshape(total_snps, BAND)
```

```python
import functools

import jax
import jax.numpy as jnp
from jax import lax
from jax.experimental import pallas as pl
from jax.experimental.pallas import tpu as pltpu
from jax.sharding import PartitionSpec as P

TILE = 512
BAND = 4096
EPS = 1e-05
CHUNK = 256
MESH = pl.DeviceIdType.MESH


def kernel(
    geno_hbm,
    out_hbm,
    geno,
    stats,
    ext,
    rows_t,
    acc,
    core_out,
    core_in,
    cross_out,
    cross_in,
    geno_sem,
    stats_send,
    stats_recv,
    back_send,
    ring_send,
    ext_recv,
    core_send,
    core_recv,
    cross_send,
    cross_recv,
    out_sem,
):
    samp = lax.axis_index("samp")
    snp = lax.axis_index("snp")
    n_snp = lax.axis_size("snp")
    half, core = samp // 2, samp % 2
    x = snp % 4
    row0 = snp - x
    has_prev = snp >= 4
    has_next = snp < n_snp - 4
    core_peer = (half * 2 + 1 - core, snp)
    cross_peer = ((1 - half) * 2 + core, snp)

    def remote(src, dst, send, recv, to):
        return pltpu.make_async_remote_copy(
            src_ref=src, dst_ref=dst, send_sem=send, recv_sem=recv, device_id=to, device_id_type=MESH
        )

    def geno_copy(c):
        return pltpu.make_async_copy(
            geno_hbm.at[:, pl.ds(c * CHUNK, CHUNK)], geno.at[c], geno_sem.at[c]
        )

    for c in range(4):
        geno_copy(c).start()

    barrier = pltpu.get_barrier_semaphore()
    for d in range(1, 4):
        pl.semaphore_signal(barrier, inc=1, device_id=((samp + d) % 4, snp), device_id_type=MESH)
        pl.semaphore_signal(barrier, inc=1, device_id=(samp, row0 + (x + d) % 4), device_id_type=MESH)

    @pl.when(has_prev)
    def _():
        pl.semaphore_signal(barrier, inc=1, device_id=(samp, snp - 4), device_id_type=MESH)

    @pl.when(has_next)
    def _():
        pl.semaphore_signal(barrier, inc=1, device_id=(samp, snp + 4), device_id_type=MESH)

    for c in range(4):
        geno_copy(c).wait()
        g = geno[c]
        dosage = jnp.maximum(g, 0.0)
        present = (g >= 0.0).astype(jnp.float32)
        cols = pl.ds(c * CHUNK, CHUNK)
        stats[samp, 0:1, cols] = jnp.sum(present, axis=0, keepdims=True)
        stats[samp, 1:2, cols] = jnp.sum(dosage, axis=0, keepdims=True)
        stats[samp, 2:3, cols] = jnp.sum(dosage * dosage, axis=0, keepdims=True)

    pl.semaphore_wait(
        barrier, 6 + has_prev.astype(jnp.int32) + has_next.astype(jnp.int32)
    )

    def stats_copy(d):
        return remote(
            stats.at[samp], stats.at[samp], stats_send.at[d - 1], stats_recv.at[samp], ((samp + d) % 4, snp)
        )

    for d in range(1, 4):
        stats_copy(d).start()

    @pl.when(jnp.logical_not(has_next))
    def _():
        for c in range(4):
            ext[16 + c] = jnp.zeros((1024, CHUNK), jnp.bfloat16)

    for d in range(1, 4):
        other = (samp + d) % 4
        remote(stats.at[other], stats.at[other], stats_send.at[d - 1], stats_recv.at[other], (other, snp)).wait_recv()

    def back_copy(c):
        return remote(ext.at[c], ext.at[16 + c], back_send.at[c], ext_recv.at[16 + c], (samp, snp - 4))

    def ring_copy(k, base, c):
        return remote(
            ext.at[base + c],
            ext.at[4 * k + c],
            ring_send.at[k - 1, c],
            ext_recv.at[4 * k + c],
            (samp, row0 + (x + 4 - k) % 4),
        )

    for c in range(4):
        cols = pl.ds(c * CHUNK, CHUNK)
        total = stats[0, 0:3, cols] + stats[1, 0:3, cols] + stats[2, 0:3, cols] + stats[3, 0:3, cols]
        counted, summed, squared = total[0:1], total[1:2], total[2:3]
        average = summed / counted
        spread = squared / counted - average * average
        col_norms = counted * spread / (spread + EPS)
        scale = lax.rsqrt(spread + EPS) * lax.rsqrt(col_norms)
        g = geno[c]
        scaled = jnp.where(g >= 0.0, (g - average) * scale, 0.0)
        ext[c] = scaled.astype(jnp.bfloat16)
        rows_t[pl.ds(c * CHUNK, CHUNK), :] = scaled.T.astype(jnp.bfloat16)

        @pl.when(has_prev & ((x < 3) | (c < 2)))
        def _():
            back_copy(c).start()

        for k in range(1, 4):

            @pl.when(x >= k)
            def _():
                ring_copy(k, 0, c).start()

    def chunk_of(i):
        j = i - 6
        b, kk = j // 3, j % 3
        k = jnp.where(kk == 0, 1, jnp.where(kk == 1, 3, 2))
        return jnp.where(i < 4, i, jnp.where(i < 6, 12 + i, 4 * k + b))

    def core_copy(u):
        return remote(core_out.at[u], core_in.at[u], core_send.at[u], core_recv.at[u], core_peer)

    def cross_copy(u):
        return remote(cross_out.at[u], cross_in.at[u], cross_send.at[u], cross_recv.at[u], cross_peer)

    def place(g, t):
        r = g - 2 * t
        q, m = r // 4, r % 4
        return (r >= 0) & (r < 16), q % 2 == core, q // 2, m

    def multiply(g):
        for t in range(2):
            valid, mine, h, m = place(g, t)

            @pl.when(valid)
            def _():
                u = (2 * t + h) * 4 + m
                part = jnp.dot(
                    rows_t[t * TILE : (t + 1) * TILE, :], ext[g], preferred_element_type=jnp.float32
                )

                @pl.when(mine)
                def _():
                    acc[u] = part

                @pl.when(jnp.logical_not(mine))
                def _():
                    core_out[u] = part.astype(jnp.bfloat16)
                    core_copy(u).start()

    def reduce(g):
        for t in range(2):
            valid, mine, h, m = place(g, t)

            @pl.when(valid & mine)
            def _():
                u = (2 * t + h) * 4 + m
                core_copy(u).wait_recv()

                @pl.when(h != half)
                def _():
                    v = t * 4 + m
                    cross_out[v] = (acc[u] + core_in[u].astype(jnp.float32)).astype(jnp.bfloat16)
                    cross_copy(v).start()

    def step(i, carry):
        @pl.when(i == 4)
        def _():
            for c in range(4):

                @pl.when(has_next & ((x < 3) | (c < 2)))
                def _():
                    back_copy(c).wait_recv()

                for k in range(1, 4):

                    @pl.when(x < k)
                    def _():
                        ring_copy(k, 16, c).start()

        @pl.when(i < 18)
        def _():
            g = chunk_of(i)

            @pl.when(i >= 6)
            def _():
                remote(ext.at[g], ext.at[g], ring_send.at[0, 0], ext_recv.at[g], core_peer).wait_recv()

            multiply(g)

        @pl.when(i > 0)
        def _():
            reduce(chunk_of(i - 1))

        return carry

    lax.fori_loop(0, 19, step, 0)

    def out_copy(v):
        t, m = v // 4, v % 4
        return pltpu.make_async_copy(
            acc.at[(2 * t + half) * 4 + m],
            out_hbm.at[pl.ds(t * TILE, TILE), pl.ds(pl.multiple_of(m * CHUNK, CHUNK), CHUNK)],
            out_sem.at[v],
        )

    def finish(v, carry):
        t, m = v // 4, v % 4
        u = (2 * t + half) * 4 + m
        cross_copy(v).wait_recv()
        acc[u] = acc[u] + core_in[u].astype(jnp.float32) + cross_in[v].astype(jnp.float32)
        out_copy(v).start()
        return carry

    lax.fori_loop(0, 8, finish, 0)

    for d in range(1, 4):
        stats_copy(d).wait_send()
    for c in range(4):

        @pl.when(has_prev & ((x < 3) | (c < 2)))
        def _():
            back_copy(c).wait_send()

        for k in range(1, 4):
            ring_copy(k, 0, c).wait_send()

    def drain_core(v, carry):
        t, hm = v // 8, v % 8
        h, m = hm // 4, hm % 4
        core_copy((2 * t + h) * 4 + m).wait_send()
        return carry

    lax.fori_loop(0, 16, drain_core, 0)

    def drain(v, carry):
        cross_copy(v).wait_send()
        out_copy(v).wait()
        return carry

    lax.fori_loop(0, 8, drain, 0)


def on_device(genotypes):
    samples, snps = genotypes.shape
    dma = pltpu.SemaphoreType.DMA
    return pl.pallas_call(
        kernel,
        out_shape=jax.ShapeDtypeStruct((snps, BAND // lax.axis_size("samp")), jnp.float32),
        in_specs=[pl.BlockSpec(memory_space=pl.ANY)],
        out_specs=pl.BlockSpec(memory_space=pl.ANY),
        scratch_shapes=[
            pltpu.VMEM((4, samples, CHUNK), jnp.float32),
            pltpu.VMEM((4, 8, snps), jnp.float32),
            pltpu.VMEM((20, samples, CHUNK), jnp.bfloat16),
            pltpu.VMEM((snps, samples), jnp.bfloat16),
            pltpu.VMEM((16, TILE, CHUNK), jnp.float32),
            pltpu.VMEM((16, TILE, CHUNK), jnp.bfloat16),
            pltpu.VMEM((16, TILE, CHUNK), jnp.bfloat16),
            pltpu.VMEM((8, TILE, CHUNK), jnp.bfloat16),
            pltpu.VMEM((8, TILE, CHUNK), jnp.bfloat16),
            dma((4,)),
            dma((3,)),
            dma((4,)),
            dma((4,)),
            dma((3, 4)),
            dma((20,)),
            dma((16,)),
            dma((16,)),
            dma((8,)),
            dma((8,)),
            dma((8,)),
        ],
        compiler_params=pltpu.CompilerParams(
            collective_id=0, has_side_effects=True, vmem_limit_bytes=60 * 2**20
        ),
        name="ld_band",
    )(genotypes)


def solution(mesh):
    return jax.shard_map(
        on_device, mesh=mesh, in_specs=(P("samp", "snp"),), out_specs=P("snp", "samp"), check_vma=False
    )
```

```python
import functools

import jax
import jax.numpy as jnp
from jax import lax
from jax.experimental import pallas as pl
from jax.experimental.pallas import tpu as pltpu
from jax.sharding import PartitionSpec as P

TILE = 512
BAND = 4096
EPS = 1e-05
CHUNK = 256
MISSING = -4.0
PRESENT = -3.0
MESH = pl.DeviceIdType.MESH
OWN = (0, 1, 2, 3)
ORDER = (
    OWN + (4, 5, 12, 6, 13, 7, 16, 17, 14, 8, 15, 9, 10, 11),
    OWN + (4, 12, 13, 8, 14, 9, 16, 17, 15, 10, 11, 5, 6, 7),
    OWN + (4, 5, 12, 6, 13, 7, 8, 9, 16, 17, 14, 15, 10, 11),
    OWN + (16, 17, 4, 5, 8, 6, 9, 7, 12, 13, 14, 15, 10, 11),
)
PASS_AT = (4, 5, 7, 9)


def look_up(i, values):
    found = values[0]
    for n, v in enumerate(values):
        if n:
            found = jnp.where(i == n, v, found)
    return found


def kernel(
    geno_hbm,
    out,
    geno,
    stats,
    ext,
    affine,
    own,
    scratch,
    rows_t,
    acc,
    core_out,
    core_in,
    cross_out,
    cross_in,
    geno_sem,
    stats_send,
    stats_recv,
    back_send,
    ring_send,
    relay_send,
    ext_recv,
    affine_send,
    affine_recv,
    core_send,
    core_recv,
    cross_send,
    cross_recv,
):
    samp = lax.axis_index("samp")
    snp = lax.axis_index("snp")
    n_snp = lax.axis_size("snp")
    half, core = samp // 2, samp % 2
    x = snp % 4
    row0 = snp - x
    has_prev = snp >= 4
    has_next = snp < n_snp - 4
    core_peer = (half * 2 + 1 - core, snp)
    cross_peer = ((1 - half) * 2 + core, snp)

    def remote(src, dst, send, recv, to):
        return pltpu.make_async_remote_copy(
            src_ref=src, dst_ref=dst, send_sem=send, recv_sem=recv, device_id=to, device_id_type=MESH
        )

    def geno_copy(c):
        return pltpu.make_async_copy(
            geno_hbm.at[:, pl.ds(c * CHUNK, CHUNK)], geno.at[c], geno_sem.at[c]
        )

    for c in range(4):
        geno_copy(c).start()

    barrier = pltpu.get_barrier_semaphore()
    for d in range(1, 4):
        pl.semaphore_signal(barrier, inc=1, device_id=((samp + d) % 4, snp), device_id_type=MESH)
        pl.semaphore_signal(barrier, inc=1, device_id=(samp, row0 + (x + d) % 4), device_id_type=MESH)

    @pl.when(has_prev)
    def _():
        pl.semaphore_signal(barrier, inc=1, device_id=(samp, snp - 4), device_id_type=MESH)

    @pl.when(has_next)
    def _():
        pl.semaphore_signal(barrier, inc=1, device_id=(samp, snp + 4), device_id_type=MESH)

    for c in range(4):
        geno_copy(c).wait()
        g = geno[c]
        dosage = jnp.maximum(g, 0.0)
        present = (g >= 0.0).astype(jnp.float32)
        cols = pl.ds(c * CHUNK, CHUNK)
        stats[samp, 0:1, cols] = jnp.sum(present, axis=0, keepdims=True)
        stats[samp, 1:2, cols] = jnp.sum(dosage, axis=0, keepdims=True)
        stats[samp, 2:3, cols] = jnp.sum(dosage * dosage, axis=0, keepdims=True)

    pl.semaphore_wait(barrier, 6 + has_prev.astype(jnp.int32) + has_next.astype(jnp.int32))

    def stats_copy(d):
        return remote(
            stats.at[samp], stats.at[samp], stats_send.at[d - 1], stats_recv.at[samp], ((samp + d) % 4, snp)
        )

    for d in range(1, 4):
        stats_copy(d).start()

    def back_copy(c):
        return remote(ext.at[c], ext.at[16 + c], back_send.at[c], ext_recv.at[16 + c], (samp, snp - 4))

    def ring_to(k):
        return (samp, row0 + (x + 4 - k) % 4)

    def ring_copy(k, base, c):
        return remote(
            ext.at[base + c], ext.at[4 * k + c], ring_send.at[k - 1, c], ext_recv.at[4 * k + c], ring_to(k)
        )

    def affine_back():
        return remote(affine.at[0], affine.at[4], affine_send.at[0], affine_recv.at[4], (samp, snp - 4))

    def affine_ring(k, base):
        return remote(affine.at[base], affine.at[k], affine_send.at[k], affine_recv.at[k], ring_to(k))

    inner = (x == 1) | (x == 2)
    late_near = (half == 0) & (x == 1)
    late_far = (half == 1) & (x == 2)

    def relay_to(k):
        return (samp, jnp.where(k == 1, snp - 1, snp + 1))

    def relay_copy(k, c):
        return remote(
            ext.at[4 * k + c], ext.at[8 + c], relay_send.at[4 * (k // 2) + c], ext_recv.at[8 + c], relay_to(k)
        )

    def affine_relay(k):
        return remote(affine.at[k], affine.at[2], affine_send.at[4 + k // 2], affine_recv.at[2], relay_to(k))

    def send_back(c):
        @pl.when(has_prev & ((x < 3) | (c < 2)))
        def _():
            back_copy(c).start()

    def send_ring(c):
        @pl.when((x >= 1) if c == 0 else ((x >= 1) & jnp.logical_not(late_near)))
        def _():
            ring_copy(1, 0, c).start()

        @pl.when(x >= 3)
        def _():
            ring_copy(3, 0, c).start()

    for c in range(4):
        cols = pl.ds(c * CHUNK, CHUNK)
        g = geno[c]
        middle = stats[samp, 1:2, cols] / stats[samp, 0:1, cols]
        ext[c] = jnp.where(g >= 0.0, g - middle, MISSING).astype(jnp.bfloat16)
        if c == 0:
            send_back(0)
            send_ring(0)

    @pl.when(jnp.logical_not(has_next))
    def _():
        affine[4] = jnp.zeros((2, 1024), jnp.float32)
        for c in range(4):
            ext[16 + c] = jnp.zeros((1024, CHUNK), jnp.bfloat16)

    for d in range(1, 4):
        other = (samp + d) % 4
        remote(stats.at[other], stats.at[other], stats_send.at[d - 1], stats_recv.at[other], (other, snp)).wait_recv()

    for c in range(4):
        cols = pl.ds(c * CHUNK, CHUNK)
        total = stats[0, 0:3, cols] + stats[1, 0:3, cols] + stats[2, 0:3, cols] + stats[3, 0:3, cols]
        counted, summed, squared = total[0:1], total[1:2], total[2:3]
        average = summed / counted
        spread = squared / counted - average * average
        col_norms = counted * spread / (spread + EPS)
        scale = lax.rsqrt(spread + EPS) * lax.rsqrt(col_norms)
        middle = stats[samp, 1:2, cols] / stats[samp, 0:1, cols]
        affine[0, 0:1, cols] = scale
        affine[0, 1:2, cols] = (middle - average) * scale

    @pl.when(has_prev)
    def _():
        affine_back().start()

    for k in (1, 3):

        @pl.when(x >= k)
        def _():
            affine_ring(k, 0).start()

    for c in range(1, 4):
        send_back(c)
        send_ring(c)

    for c in range(4):
        cols = pl.ds(c * CHUNK, CHUNK)
        scale, shift = affine[0, 0:1, cols], affine[0, 1:2, cols]
        middle = stats[samp, 1:2, cols] / stats[samp, 0:1, cols]
        g = geno[c]
        scaled = jnp.where(g >= 0.0, (g - middle) * scale + shift, 0.0)
        own[c] = scaled.astype(jnp.bfloat16)
        rows_t[pl.ds(c * CHUNK, CHUNK), :] = scaled.T.astype(jnp.bfloat16)

    def chunk_of(i):
        g = [look_up(i, order) for order in ORDER]
        return jnp.where(half == 0, jnp.where(x == 0, g[1], g[0]), jnp.where(x == 3, g[3], g[2]))

    def core_copy(u):
        return remote(core_out.at[u], core_in.at[u], core_send.at[u], core_recv.at[u], core_peer)

    def cross_copy(u):
        return remote(cross_out.at[u], cross_in.at[u], cross_send.at[u], cross_recv.at[u], cross_peer)

    def place(g, t):
        r = g - 2 * t
        q, m = r // 4, r % 4
        return (r >= 0) & (r < 16), q % 2 == core, q // 2, m

    def multiply(g, block):
        for t in range(2):
            valid, mine, h, m = place(g, t)

            @pl.when(valid)
            def _():
                u = (2 * t + h) * 4 + m
                part = jnp.dot(
                    rows_t[t * TILE : (t + 1) * TILE, :], block[...], preferred_element_type=jnp.float32
                )

                @pl.when(mine)
                def _():
                    acc[u] = part

                @pl.when(jnp.logical_not(mine))
                def _():
                    core_out[u] = part.astype(jnp.bfloat16)
                    core_copy(u).start()

    def reduce(g):
        for t in range(2):
            valid, mine, h, m = place(g, t)

            @pl.when(valid & mine)
            def _():
                u = (2 * t + h) * 4 + m
                core_copy(u).wait_recv()

                @pl.when(h != half)
                def _():
                    v = t * 4 + m
                    cross_out[v] = (acc[u] + core_in[u].astype(jnp.float32)).astype(jnp.bfloat16)
                    cross_copy(v).start()

    def step(i, carry):
        for c in range(4):

            @pl.when(i == PASS_AT[c])
            def _():
                @pl.when(has_next & ((x < 3) | (c < 2)))
                def _():
                    back_copy(c).wait_recv()

                @pl.when(x < 1)
                def _():
                    ring_copy(1, 16, c).start()

                @pl.when((x < 3) if c == 3 else ((x < 3) & jnp.logical_not(late_far)))
                def _():
                    ring_copy(3, 16, c).start()

                if c == 0:

                    @pl.when(has_next)
                    def _():
                        affine_back().wait_recv()

                    for k in (1, 3):

                        @pl.when(x < k)
                        def _():
                            affine_ring(k, 4).start()

        @pl.when(i < 4)
        def _():
            multiply(i, own.at[i])

        @pl.when((i >= 4) & (i < 18))
        def _():
            g = chunk_of(i)
            k, b = g // 4, g % 4

            @pl.when(k < 4)
            def _():
                remote(ext.at[g], ext.at[g], ring_send.at[0, 0], ext_recv.at[g], core_peer).wait_recv()

                @pl.when(inner & (k != 2))
                def _():
                    relay_copy(k, b).start()

                @pl.when(b == 0)
                def _():
                    affine_ring(k, 0).wait_recv()

                    @pl.when(inner & (k != 2))
                    def _():
                        affine_relay(k).start()

                @pl.when(late_near & (g == 7))
                def _():
                    for c in range(1, 4):
                        ring_copy(1, 0, c).start()

                @pl.when(late_far & (g == 13))
                def _():
                    for c in range(3):
                        ring_copy(3, 16, c).start()

            v = ext[g].astype(jnp.float32)
            cols = pl.ds(pl.multiple_of(b * CHUNK, CHUNK), CHUNK)
            scale, shift = affine[k, 0:1, cols], affine[k, 1:2, cols]
            scratch[...] = jnp.where(v > PRESENT, v * scale + shift, 0.0).astype(jnp.bfloat16)
            multiply(g, scratch)

        @pl.when(i > 0)
        def _():
            reduce(chunk_of(i - 1))

        return carry

    lax.fori_loop(0, 19, step, 0)

    def finish(v, carry):
        t, m = v // 4, v % 4
        u = (2 * t + half) * 4 + m
        cross_copy(v).wait_recv()
        rows, cols = pl.ds(pl.multiple_of(t * TILE, TILE), TILE), pl.ds(pl.multiple_of(m * CHUNK, CHUNK), CHUNK)
        out[rows, cols] = acc[u] + core_in[u].astype(jnp.float32) + cross_in[v].astype(jnp.float32)
        return carry

    lax.fori_loop(0, 8, finish, 0)

    for d in range(1, 4):
        stats_copy(d).wait_send()
    for c in range(4):

        @pl.when(has_prev & ((x < 3) | (c < 2)))
        def _():
            back_copy(c).wait_send()

        for k in (1, 3):
            ring_copy(k, 0, c).wait_send()

            @pl.when(inner)
            def _():
                relay_copy(k, c).wait_send()

    @pl.when(has_prev)
    def _():
        affine_back().wait_send()

    for k in (1, 3):
        affine_ring(k, 0).wait_send()

        @pl.when(inner)
        def _():
            affine_relay(k).wait_send()

    def drain_core(v, carry):
        t, hm = v // 8, v % 8
        h, m = hm // 4, hm % 4
        core_copy((2 * t + h) * 4 + m).wait_send()
        return carry

    lax.fori_loop(0, 16, drain_core, 0)

    def drain(v, carry):
        cross_copy(v).wait_send()
        return carry

    lax.fori_loop(0, 8, drain, 0)


def on_device(genotypes):
    samples, snps = genotypes.shape
    dma = pltpu.SemaphoreType.DMA
    return pl.pallas_call(
        kernel,
        out_shape=jax.ShapeDtypeStruct((snps, BAND // lax.axis_size("samp")), jnp.float32),
        in_specs=[pl.BlockSpec(memory_space=pltpu.HBM)],
        out_specs=pl.BlockSpec(memory_space=pltpu.VMEM),
        scratch_shapes=[
            pltpu.VMEM((4, samples, CHUNK), jnp.float32),
            pltpu.VMEM((4, 8, snps), jnp.float32),
            pltpu.VMEM((20, samples, CHUNK), jnp.bfloat16),
            pltpu.VMEM((5, 2, snps), jnp.float32),
            pltpu.VMEM((4, samples, CHUNK), jnp.bfloat16),
            pltpu.VMEM((samples, CHUNK), jnp.bfloat16),
            pltpu.VMEM((snps, samples), jnp.bfloat16),
            pltpu.VMEM((16, TILE, CHUNK), jnp.float32),
            pltpu.VMEM((16, TILE, CHUNK), jnp.bfloat16),
            pltpu.VMEM((16, TILE, CHUNK), jnp.bfloat16),
            pltpu.VMEM((8, TILE, CHUNK), jnp.bfloat16),
            pltpu.VMEM((8, TILE, CHUNK), jnp.bfloat16),
            dma((4,)),
            dma((3,)),
            dma((4,)),
            dma((4,)),
            dma((3, 4)),
            dma((8,)),
            dma((20,)),
            dma((6,)),
            dma((5,)),
            dma((16,)),
            dma((16,)),
            dma((8,)),
            dma((8,)),
        ],
        compiler_params=pltpu.CompilerParams(
            collective_id=0, has_side_effects=True, vmem_limit_bytes=47 * 2**20
        ),
        name="ld_band",
    )(genotypes)


def solution(mesh):
    return jax.shard_map(
        on_device, mesh=mesh, in_specs=(P("samp", "snp"),), out_specs=P("snp", "samp"), check_vma=False
    )
```

```python
import functools

import jax
import jax.numpy as jnp
from jax import lax
from jax.experimental import pallas as pl
from jax.experimental.pallas import tpu as pltpu
from jax.sharding import PartitionSpec as P

TILE = 512
BAND = 4096
EPS = 1e-05
CHUNK = 256
MISSING = -4.0
PRESENT = -3.0
MESH = pl.DeviceIdType.MESH
OWN = (0, 1, 2, 3)
ORDER = (
    (
        OWN + (12, 16, 13, 17, 14, 8, 15, 9, 10, 11, 4, 5, 6, 7),
        OWN + (4, 16, 5, 17, 6, 12, 7, 13, 8, 14, 9, 15, 10, 11),
        OWN + (4, 16, 5, 12, 6, 13, 7, 17, 8, 14, 9, 15, 10, 11),
        OWN + (16, 4, 17, 12, 5, 8, 13, 6, 9, 14, 7, 15, 10, 11),
    ),
    (
        OWN + (4, 5, 6, 8, 7, 9, 16, 17, 12, 13, 14, 15, 10, 11),
        OWN + (4, 5, 6, 16, 7, 17, 8, 9, 12, 13, 14, 15, 10, 11),
        OWN + (4, 5, 12, 6, 13, 7, 8, 9, 16, 17, 14, 15, 10, 11),
        OWN + (16, 4, 17, 5, 8, 6, 9, 7, 12, 13, 14, 15, 10, 11),
    ),
)
PASS_AT = (4, 6, 8, 10)


def look_up(i, values):
    found = values[0]
    for n, v in enumerate(values):
        if n:
            found = jnp.where(i == n, v, found)
    return found


def kernel(
    geno_hbm,
    out,
    geno,
    stats,
    ext,
    affine,
    own,
    scratch,
    rows_t,
    acc,
    core_out,
    core_in,
    cross_out,
    cross_in,
    geno_sem,
    stats_send,
    stats_recv,
    back_send,
    ring_send,
    relay_send,
    ext_recv,
    affine_send,
    affine_recv,
    core_send,
    core_recv,
    cross_send,
    cross_recv,
):
    samp = lax.axis_index("samp")
    snp = lax.axis_index("snp")
    n_snp = lax.axis_size("snp")
    half, core = samp // 2, samp % 2
    x = snp % 4
    row0 = snp - x
    has_prev = snp >= 4
    has_next = snp < n_snp - 4
    core_peer = (half * 2 + 1 - core, snp)
    cross_peer = ((1 - half) * 2 + core, snp)

    def remote(src, dst, send, recv, to):
        return pltpu.make_async_remote_copy(
            src_ref=src, dst_ref=dst, send_sem=send, recv_sem=recv, device_id=to, device_id_type=MESH
        )

    def geno_copy(c):
        return pltpu.make_async_copy(
            geno_hbm.at[:, pl.ds(c * CHUNK, CHUNK)], geno.at[c], geno_sem.at[c]
        )

    for c in range(4):
        geno_copy(c).start()

    barrier = pltpu.get_barrier_semaphore()
    for d in range(1, 4):
        pl.semaphore_signal(barrier, inc=1, device_id=((samp + d) % 4, snp), device_id_type=MESH)
        pl.semaphore_signal(barrier, inc=1, device_id=(samp, row0 + (x + d) % 4), device_id_type=MESH)

    @pl.when(has_prev)
    def _():
        pl.semaphore_signal(barrier, inc=1, device_id=(samp, snp - 4), device_id_type=MESH)

    @pl.when(has_next)
    def _():
        pl.semaphore_signal(barrier, inc=1, device_id=(samp, snp + 4), device_id_type=MESH)

    for c in range(4):
        geno_copy(c).wait()
        g = geno[c]
        dosage = jnp.maximum(g, 0.0)
        present = (g >= 0.0).astype(jnp.float32)
        cols = pl.ds(c * CHUNK, CHUNK)
        stats[samp, 0:1, cols] = jnp.sum(present, axis=0, keepdims=True)
        stats[samp, 1:2, cols] = jnp.sum(dosage, axis=0, keepdims=True)
        stats[samp, 2:3, cols] = jnp.sum(dosage * dosage, axis=0, keepdims=True)

    pl.semaphore_wait(barrier, 6 + has_prev.astype(jnp.int32) + has_next.astype(jnp.int32))

    def stats_copy(d):
        return remote(
            stats.at[samp], stats.at[samp], stats_send.at[d - 1], stats_recv.at[samp], ((samp + d) % 4, snp)
        )

    for d in range(1, 4):
        stats_copy(d).start()

    def back_copy(c):
        return remote(ext.at[c], ext.at[16 + c], back_send.at[c], ext_recv.at[16 + c], (samp, snp - 4))

    def ring_to(k):
        return (samp, row0 + (x + 4 - k) % 4)

    def ring_copy(k, base, c):
        return remote(
            ext.at[base + c], ext.at[4 * k + c], ring_send.at[k - 1, c], ext_recv.at[4 * k + c], ring_to(k)
        )

    def affine_back():
        return remote(affine.at[0], affine.at[4], affine_send.at[0], affine_recv.at[4], (samp, snp - 4))

    def affine_ring(k, base):
        return remote(affine.at[base], affine.at[k], affine_send.at[k], affine_recv.at[k], ring_to(k))

    def relays(k, c):
        return ((k == 1) & (x >= 1)) | ((k == 3) & (x == 2))

    def relays_affine(k):
        return ((k == 1) & (x >= 1)) | ((k == 3) & (x == 2))

    late_near = (half == 0) & (x == 1)
    late_far = (half == 1) & (x == 2)

    def relay_to(k):
        return (samp, jnp.where(k == 1, snp - 1, snp + 1))

    def relay_copy(k, c):
        return remote(
            ext.at[4 * k + c], ext.at[8 + c], relay_send.at[4 * (k // 2) + c], ext_recv.at[8 + c], relay_to(k)
        )

    def affine_relay(k):
        return remote(affine.at[k], affine.at[2], affine_send.at[4 + k // 2], affine_recv.at[2], relay_to(k))

    def send_back(c):
        @pl.when(has_prev & ((x < 3) | (c < 2)))
        def _():
            back_copy(c).start()

    def send_ring(c):
        @pl.when((x >= 1) if c < 2 else ((x >= 1) & jnp.logical_not(late_near)))
        def _():
            ring_copy(1, 0, c).start()

        @pl.when(x >= 3)
        def _():
            ring_copy(3, 0, c).start()

    for c in range(4):
        cols = pl.ds(c * CHUNK, CHUNK)
        g = geno[c]
        middle = stats[samp, 1:2, cols] / stats[samp, 0:1, cols]
        ext[c] = jnp.where(g >= 0.0, g - middle, MISSING).astype(jnp.bfloat16)
        if c == 0:
            send_back(0)
            send_ring(0)

    @pl.when(jnp.logical_not(has_next))
    def _():
        affine[4] = jnp.zeros((2, 1024), jnp.float32)
        for c in range(4):
            ext[16 + c] = jnp.zeros((1024, CHUNK), jnp.bfloat16)

    for d in range(1, 4):
        other = (samp + d) % 4
        remote(stats.at[other], stats.at[other], stats_send.at[d - 1], stats_recv.at[other], (other, snp)).wait_recv()

    for c in range(4):
        cols = pl.ds(c * CHUNK, CHUNK)
        total = stats[0, 0:3, cols] + stats[1, 0:3, cols] + stats[2, 0:3, cols] + stats[3, 0:3, cols]
        counted, summed, squared = total[0:1], total[1:2], total[2:3]
        average = summed / counted
        spread = squared / counted - average * average
        col_norms = counted * spread / (spread + EPS)
        scale = lax.rsqrt(spread + EPS) * lax.rsqrt(col_norms)
        middle = stats[samp, 1:2, cols] / stats[samp, 0:1, cols]
        affine[0, 0:1, cols] = scale
        affine[0, 1:2, cols] = (middle - average) * scale

    @pl.when(has_prev)
    def _():
        affine_back().start()

    for k in (1, 3):

        @pl.when(x >= k)
        def _():
            affine_ring(k, 0).start()


    for c in range(1, 4):
        send_back(c)
        send_ring(c)

    for c in range(4):
        cols = pl.ds(c * CHUNK, CHUNK)
        scale, shift = affine[0, 0:1, cols], affine[0, 1:2, cols]
        middle = stats[samp, 1:2, cols] / stats[samp, 0:1, cols]
        g = geno[c]
        scaled = jnp.where(g >= 0.0, (g - middle) * scale + shift, 0.0)
        own[c] = scaled.astype(jnp.bfloat16)
        rows_t[pl.ds(c * CHUNK, CHUNK), :] = scaled.T.astype(jnp.bfloat16)

    def chunk_of(i):
        g = [look_up(x, [look_up(i, order) for order in orders]) for orders in ORDER]
        return jnp.where(half == 0, g[0], g[1])

    def core_copy(u):
        return remote(core_out.at[u], core_in.at[u], core_send.at[u], core_recv.at[u], core_peer)

    def cross_copy(u):
        return remote(cross_out.at[u], cross_in.at[u], cross_send.at[u], cross_recv.at[u], cross_peer)

    def place(g, t):
        r = g - 2 * t
        q, m = r // 4, r % 4
        return (r >= 0) & (r < 16), q % 2 == core, q // 2, m

    def multiply(g, block):
        for t in range(2):
            valid, mine, h, m = place(g, t)

            @pl.when(valid)
            def _():
                u = (2 * t + h) * 4 + m
                part = jnp.dot(
                    rows_t[t * TILE : (t + 1) * TILE, :], block[...], preferred_element_type=jnp.float32
                )

                @pl.when(mine)
                def _():
                    acc[u] = part

                @pl.when(jnp.logical_not(mine))
                def _():
                    core_out[u] = part.astype(jnp.bfloat16)
                    core_copy(u).start()

    def reduce(g):
        for t in range(2):
            valid, mine, h, m = place(g, t)

            @pl.when(valid & mine)
            def _():
                u = (2 * t + h) * 4 + m
                core_copy(u).wait_recv()

                @pl.when(h != half)
                def _():
                    v = t * 4 + m
                    cross_out[v] = (acc[u] + core_in[u].astype(jnp.float32)).astype(jnp.bfloat16)
                    cross_copy(v).start()

    def step(i, carry):
        for c in range(4):

            @pl.when(i == PASS_AT[c])
            def _():
                @pl.when(has_next & ((x < 3) | (c < 2)))
                def _():
                    back_copy(c).wait_recv()

                @pl.when(x < 1)
                def _():
                    ring_copy(1, 16, c).start()

                @pl.when((x < 3) if c == 3 else ((x < 3) & jnp.logical_not(late_far)))
                def _():
                    ring_copy(3, 16, c).start()

                if c == 0:

                    @pl.when(has_next)
                    def _():
                        affine_back().wait_recv()

                    for k in (1, 3):

                        @pl.when(x < k)
                        def _():
                            affine_ring(k, 4).start()

        @pl.when(i < 4)
        def _():
            multiply(i, own.at[i])

        @pl.when((i >= 4) & (i < 18))
        def _():
            g = chunk_of(i)
            k, b = g // 4, g % 4

            @pl.when(k < 4)
            def _():
                remote(ext.at[g], ext.at[g], ring_send.at[0, 0], ext_recv.at[g], core_peer).wait_recv()

                @pl.when(relays(k, b))
                def _():
                    relay_copy(k, b).start()

                @pl.when(b == 0)
                def _():
                    affine_ring(k, 0).wait_recv()

                    @pl.when(relays_affine(k))
                    def _():
                        affine_relay(k).start()

                @pl.when(late_near & (g == 7))
                def _():
                    for c in range(2, 4):
                        ring_copy(1, 0, c).start()

                @pl.when(late_far & (g == 13))
                def _():
                    for c in range(3):
                        ring_copy(3, 16, c).start()

            v = ext[g].astype(jnp.float32)
            cols = pl.ds(pl.multiple_of(b * CHUNK, CHUNK), CHUNK)
            scale, shift = affine[k, 0:1, cols], affine[k, 1:2, cols]
            scratch[...] = jnp.where(v > PRESENT, v * scale + shift, 0.0).astype(jnp.bfloat16)
            multiply(g, scratch)

        @pl.when(i > 0)
        def _():
            reduce(chunk_of(i - 1))

        return carry

    lax.fori_loop(0, 19, step, 0)

    def finish(v, carry):
        t, m = v // 4, v % 4
        u = (2 * t + half) * 4 + m
        cross_copy(v).wait_recv()
        rows, cols = pl.ds(pl.multiple_of(t * TILE, TILE), TILE), pl.ds(pl.multiple_of(m * CHUNK, CHUNK), CHUNK)
        out[rows, cols] = acc[u] + core_in[u].astype(jnp.float32) + cross_in[v].astype(jnp.float32)
        return carry

    lax.fori_loop(0, 8, finish, 0)

    for d in range(1, 4):
        stats_copy(d).wait_send()
    for c in range(4):

        @pl.when(has_prev & ((x < 3) | (c < 2)))
        def _():
            back_copy(c).wait_send()

        for k in (1, 3):
            ring_copy(k, 0, c).wait_send()

            @pl.when(relays(k, c))
            def _():
                relay_copy(k, c).wait_send()


    @pl.when(has_prev)
    def _():
        affine_back().wait_send()

    for k in (1, 3):
        affine_ring(k, 0).wait_send()

        @pl.when(relays_affine(k))
        def _():
            affine_relay(k).wait_send()


    def drain_core(v, carry):
        t, hm = v // 8, v % 8
        h, m = hm // 4, hm % 4
        core_copy((2 * t + h) * 4 + m).wait_send()
        return carry

    lax.fori_loop(0, 16, drain_core, 0)

    def drain(v, carry):
        cross_copy(v).wait_send()
        return carry

    lax.fori_loop(0, 8, drain, 0)


def on_device(genotypes):
    samples, snps = genotypes.shape
    dma = pltpu.SemaphoreType.DMA
    return pl.pallas_call(
        kernel,
        out_shape=jax.ShapeDtypeStruct((snps, BAND // lax.axis_size("samp")), jnp.float32),
        in_specs=[pl.BlockSpec(memory_space=pltpu.HBM)],
        out_specs=pl.BlockSpec(memory_space=pltpu.VMEM),
        scratch_shapes=[
            pltpu.VMEM((4, samples, CHUNK), jnp.float32),
            pltpu.VMEM((4, 8, snps), jnp.float32),
            pltpu.VMEM((20, samples, CHUNK), jnp.bfloat16),
            pltpu.VMEM((5, 2, snps), jnp.float32),
            pltpu.VMEM((4, samples, CHUNK), jnp.bfloat16),
            pltpu.VMEM((samples, CHUNK), jnp.bfloat16),
            pltpu.VMEM((snps, samples), jnp.bfloat16),
            pltpu.VMEM((16, TILE, CHUNK), jnp.float32),
            pltpu.VMEM((16, TILE, CHUNK), jnp.bfloat16),
            pltpu.VMEM((16, TILE, CHUNK), jnp.bfloat16),
            pltpu.VMEM((8, TILE, CHUNK), jnp.bfloat16),
            pltpu.VMEM((8, TILE, CHUNK), jnp.bfloat16),
            dma((4,)),
            dma((3,)),
            dma((4,)),
            dma((4,)),
            dma((3, 4)),
            dma((8,)),
            dma((20,)),
            dma((6,)),
            dma((5,)),
            dma((16,)),
            dma((16,)),
            dma((8,)),
            dma((8,)),
        ],
        compiler_params=pltpu.CompilerParams(
            collective_id=0, has_side_effects=True, vmem_limit_bytes=47 * 2**20
        ),
        name="ld_band",
    )(genotypes)


def solution(mesh):
    return jax.shard_map(
        on_device, mesh=mesh, in_specs=(P("samp", "snp"),), out_specs=P("snp", "samp"), check_vma=False
    )
```

```python
import functools

import jax
import jax.numpy as jnp
from jax import lax
from jax.experimental import pallas as pl
from jax.experimental.pallas import tpu as pltpu
from jax.sharding import PartitionSpec as P

TILE = 512
BAND = 4096
EPS = 1e-05
CHUNK = 256
MISSING = -4.0
PRESENT = -3.0
MESH = pl.DeviceIdType.MESH
OWN = (0, 1, 2, 3)
ORDER = (
    (
        OWN + (12, 16, 13, 17, 14, 8, 15, 9, 10, 11, 4, 5, 6, 7),
        OWN + (4, 16, 5, 17, 6, 12, 7, 13, 8, 14, 9, 15, 10, 11),
        OWN + (4, 16, 5, 12, 6, 13, 7, 17, 8, 14, 9, 15, 10, 11),
        OWN + (16, 4, 17, 12, 5, 8, 13, 6, 9, 14, 7, 15, 10, 11),
    ),
    (
        OWN + (4, 5, 6, 8, 7, 9, 16, 17, 12, 13, 14, 15, 10, 11),
        OWN + (4, 5, 6, 16, 7, 17, 8, 9, 12, 13, 14, 15, 10, 11),
        OWN + (4, 5, 12, 6, 13, 7, 8, 9, 16, 17, 14, 15, 10, 11),
        OWN + (16, 4, 17, 5, 8, 6, 9, 7, 12, 13, 14, 15, 10, 11),
    ),
)
PASS_AT = (4, 6, 8, 10)


def look_up(i, values):
    found = values[0]
    for n, v in enumerate(values):
        if n:
            found = jnp.where(i == n, v, found)
    return found


def kernel(
    geno_hbm,
    out,
    geno,
    stats,
    ext,
    affine,
    own,
    scratch,
    rows_t,
    acc,
    core_out,
    core_in,
    cross_out,
    cross_in,
    geno_sem,
    stats_send,
    stats_recv,
    back_send,
    ring_send,
    relay_send,
    ext_recv,
    affine_send,
    affine_recv,
    core_send,
    core_recv,
    cross_send,
    cross_recv,
):
    samp = lax.axis_index("samp")
    snp = lax.axis_index("snp")
    n_snp = lax.axis_size("snp")
    half, core = samp // 2, samp % 2
    x = snp % 4
    row0 = snp - x
    has_prev = snp >= 4
    has_next = snp < n_snp - 4
    core_peer = (half * 2 + 1 - core, snp)
    cross_peer = ((1 - half) * 2 + core, snp)

    def remote(src, dst, send, recv, to):
        return pltpu.make_async_remote_copy(
            src_ref=src, dst_ref=dst, send_sem=send, recv_sem=recv, device_id=to, device_id_type=MESH
        )

    def geno_copy(c):
        return pltpu.make_async_copy(
            geno_hbm.at[:, pl.ds(c * CHUNK, CHUNK)], geno.at[c], geno_sem.at[c]
        )

    for c in range(4):
        geno_copy(c).start()

    barrier = pltpu.get_barrier_semaphore()
    for d in range(1, 4):
        pl.semaphore_signal(barrier, inc=1, device_id=((samp + d) % 4, snp), device_id_type=MESH)
        pl.semaphore_signal(barrier, inc=1, device_id=(samp, row0 + (x + d) % 4), device_id_type=MESH)

    @pl.when(has_prev)
    def _():
        pl.semaphore_signal(barrier, inc=1, device_id=(samp, snp - 4), device_id_type=MESH)

    @pl.when(has_next)
    def _():
        pl.semaphore_signal(barrier, inc=1, device_id=(samp, snp + 4), device_id_type=MESH)

    for c in range(4):
        geno_copy(c).wait()
        g = geno[c]
        dosage = jnp.maximum(g, 0.0)
        present = (g >= 0.0).astype(jnp.float32)
        cols = pl.ds(c * CHUNK, CHUNK)
        stats[samp, 0:1, cols] = jnp.sum(present, axis=0, keepdims=True)
        stats[samp, 1:2, cols] = jnp.sum(dosage, axis=0, keepdims=True)
        stats[samp, 2:3, cols] = jnp.sum(dosage * dosage, axis=0, keepdims=True)

    pl.semaphore_wait(barrier, 6 + has_prev.astype(jnp.int32) + has_next.astype(jnp.int32))

    def stats_copy(d):
        return remote(
            stats.at[samp], stats.at[samp], stats_send.at[d - 1], stats_recv.at[samp], ((samp + d) % 4, snp)
        )

    for d in range(1, 4):
        stats_copy(d).start()

    def back_copy(c):
        return remote(ext.at[c], ext.at[16 + c], back_send.at[c], ext_recv.at[16 + c], (samp, snp - 4))

    def ring_to(k):
        return (samp, row0 + (x + 4 - k) % 4)

    def ring_copy(k, base, c):
        return remote(
            ext.at[base + c], ext.at[4 * k + c], ring_send.at[k - 1, c], ext_recv.at[4 * k + c], ring_to(k)
        )

    def affine_back():
        return remote(affine.at[0], affine.at[4], affine_send.at[0], affine_recv.at[4], (samp, snp - 4))

    def affine_ring(k, base):
        return remote(affine.at[base], affine.at[k], affine_send.at[k], affine_recv.at[k], ring_to(k))

    def relays(k, c):
        return ((k == 1) & (x >= 1)) | ((k == 3) & (x == 2))

    def relays_affine(k):
        return ((k == 1) & (x >= 1)) | ((k == 3) & (x == 2))

    late_near = (half == 0) & (x == 1)
    late_far = (half == 1) & (x == 2)

    def relay_to(k):
        return (samp, jnp.where(k == 1, snp - 1, snp + 1))

    def relay_copy(k, c):
        return remote(
            ext.at[4 * k + c], ext.at[8 + c], relay_send.at[4 * (k // 2) + c], ext_recv.at[8 + c], relay_to(k)
        )

    def affine_relay(k):
        return remote(affine.at[k], affine.at[2], affine_send.at[4 + k // 2], affine_recv.at[2], relay_to(k))

    def send_back(c):
        @pl.when(has_prev & ((x < 3) | (c < 2)))
        def _():
            back_copy(c).start()

    def send_ring(c):
        @pl.when((x >= 1) if c < 2 else ((x >= 1) & jnp.logical_not(late_near)))
        def _():
            ring_copy(1, 0, c).start()

        @pl.when(x >= 3)
        def _():
            ring_copy(3, 0, c).start()

    for c in range(4):
        cols = pl.ds(c * CHUNK, CHUNK)
        g = geno[c]
        middle = stats[samp, 1:2, cols] / stats[samp, 0:1, cols]
        ext[c] = jnp.where(g >= 0.0, g - middle, MISSING).astype(jnp.bfloat16)
        if c == 0:
            send_back(0)
            send_ring(0)

    @pl.when(jnp.logical_not(has_next))
    def _():
        affine[4] = jnp.zeros((2, 1024), jnp.float32)
        for c in range(4):
            ext[16 + c] = jnp.zeros((1024, CHUNK), jnp.bfloat16)

    for d in range(1, 4):
        other = (samp + d) % 4
        remote(stats.at[other], stats.at[other], stats_send.at[d - 1], stats_recv.at[other], (other, snp)).wait_recv()

    for c in range(4):
        cols = pl.ds(c * CHUNK, CHUNK)
        total = stats[0, 0:3, cols] + stats[1, 0:3, cols] + stats[2, 0:3, cols] + stats[3, 0:3, cols]
        counted, summed, squared = total[0:1], total[1:2], total[2:3]
        average = summed / counted
        spread = squared / counted - average * average
        col_norms = counted * spread / (spread + EPS)
        scale = lax.rsqrt(spread + EPS) * lax.rsqrt(col_norms)
        middle = stats[samp, 1:2, cols] / stats[samp, 0:1, cols]
        affine[0, 0:1, cols] = scale
        affine[0, 1:2, cols] = (middle - average) * scale

    @pl.when(has_prev)
    def _():
        affine_back().start()

    for k in (1, 3):

        @pl.when(x >= k)
        def _():
            affine_ring(k, 0).start()


    for c in range(1, 4):
        send_back(c)
        send_ring(c)

    for c in range(4):
        cols = pl.ds(c * CHUNK, CHUNK)
        scale, shift = affine[0, 0:1, cols], affine[0, 1:2, cols]
        middle = stats[samp, 1:2, cols] / stats[samp, 0:1, cols]
        g = geno[c]
        scaled = jnp.where(g >= 0.0, (g - middle) * scale + shift, 0.0)
        own[c] = scaled.astype(jnp.bfloat16)
        rows_t[pl.ds(c * CHUNK, CHUNK), :] = scaled.T.astype(jnp.bfloat16)

    def chunk_of(i):
        g = [look_up(x, [look_up(i, order) for order in orders]) for orders in ORDER]
        return jnp.where(half == 0, g[0], g[1])

    def core_copy(u):
        return remote(core_out.at[u], core_in.at[u], core_send.at[u], core_recv.at[u], core_peer)

    def cross_copy(u):
        return remote(cross_out.at[u], cross_in.at[u], cross_send.at[u], cross_recv.at[u], cross_peer)

    sends_mirror = (half == 1) & (core == 0)
    has_mirror = (half == 0) & (core == 0)
    upper = pl.ds(0, TILE // 2)

    def upper_copy(u):
        return remote(
            cross_out.at[u, upper], cross_in.at[u, upper], cross_send.at[u], cross_recv.at[u], cross_peer
        )

    def place(g, t):
        r = g - 2 * t
        q, m = r // 4, r % 4
        return (r >= 0) & (r < 16), q % 2 == core, q // 2, m

    def multiply(g, block):
        for t in range(2):
            valid, mine, h, m = place(g, t)

            @pl.when(valid)
            def _():
                u = (2 * t + h) * 4 + m
                part = jnp.dot(
                    rows_t[t * TILE : (t + 1) * TILE, :], block[...], preferred_element_type=jnp.float32
                )

                @pl.when(mine)
                def _():
                    acc[u] = part

                @pl.when(jnp.logical_not(mine))
                def _():
                    core_out[u] = part.astype(jnp.bfloat16)
                    core_copy(u).start()

    def reduce(g):
        for t in range(2):
            valid, mine, h, m = place(g, t)

            @pl.when(valid & mine)
            def _():
                u = (2 * t + h) * 4 + m
                core_copy(u).wait_recv()

                @pl.when(h != half)
                def _():
                    v = t * 4 + m
                    cross_out[v] = (acc[u] + core_in[u].astype(jnp.float32)).astype(jnp.bfloat16)

                    @pl.when(sends_mirror & (m == 0))
                    def _():
                        upper_copy(v).start()

                    @pl.when(jnp.logical_not(sends_mirror & (m == 0)))
                    def _():
                        cross_copy(v).start()

    def step(i, carry):
        for c in range(4):

            @pl.when(i == PASS_AT[c])
            def _():
                @pl.when(has_next & ((x < 3) | (c < 2)))
                def _():
                    back_copy(c).wait_recv()

                @pl.when(x < 1)
                def _():
                    ring_copy(1, 16, c).start()

                @pl.when((x < 3) if c == 3 else ((x < 3) & jnp.logical_not(late_far)))
                def _():
                    ring_copy(3, 16, c).start()

                if c == 0:

                    @pl.when(has_next)
                    def _():
                        affine_back().wait_recv()

                    for k in (1, 3):

                        @pl.when(x < k)
                        def _():
                            affine_ring(k, 4).start()

        @pl.when(i < 4)
        def _():
            multiply(i, own.at[i])

        @pl.when((i >= 4) & (i < 18))
        def _():
            g = chunk_of(i)
            k, b = g // 4, g % 4

            @pl.when(k < 4)
            def _():
                remote(ext.at[g], ext.at[g], ring_send.at[0, 0], ext_recv.at[g], core_peer).wait_recv()

                @pl.when(relays(k, b))
                def _():
                    relay_copy(k, b).start()

                @pl.when(b == 0)
                def _():
                    affine_ring(k, 0).wait_recv()

                    @pl.when(relays_affine(k))
                    def _():
                        affine_relay(k).start()

                @pl.when(late_near & (g == 7))
                def _():
                    for c in range(2, 4):
                        ring_copy(1, 0, c).start()

                @pl.when(late_far & (g == 13))
                def _():
                    for c in range(3):
                        ring_copy(3, 16, c).start()

            v = ext[g].astype(jnp.float32)
            cols = pl.ds(pl.multiple_of(b * CHUNK, CHUNK), CHUNK)
            scale, shift = affine[k, 0:1, cols], affine[k, 1:2, cols]
            scratch[...] = jnp.where(v > PRESENT, v * scale + shift, 0.0).astype(jnp.bfloat16)
            multiply(g, scratch)

        @pl.when(i > 0)
        def _():
            reduce(chunk_of(i - 1))

        return carry

    lax.fori_loop(0, 19, step, 0)

    def finish(v, carry):
        t, m = v // 4, v % 4
        u = (2 * t + half) * 4 + m
        cols = pl.ds(pl.multiple_of(m * CHUNK, CHUNK), CHUNK)

        @pl.when(has_mirror & (m == 0))
        def _():
            upper_copy(v).wait_recv()
            rows = pl.ds(pl.multiple_of(t * TILE, TILE), TILE // 2)
            out[rows, cols] = (
                acc[u, upper] + core_in[u, upper].astype(jnp.float32) + cross_in[v, upper].astype(jnp.float32)
            )

        @pl.when(jnp.logical_not(has_mirror & (m == 0)))
        def _():
            cross_copy(v).wait_recv()
            rows = pl.ds(pl.multiple_of(t * TILE, TILE), TILE)
            out[rows, cols] = acc[u] + core_in[u].astype(jnp.float32) + cross_in[v].astype(jnp.float32)

        @pl.when(has_mirror & (m == 1))
        def _():
            rows = pl.ds(pl.multiple_of(t * TILE, TILE), TILE // 2)
            low = pl.ds(pl.multiple_of(t * TILE + TILE // 2, TILE // 2), TILE // 2)
            out[low, pl.ds(0, CHUNK)] = out[rows, pl.ds(CHUNK, CHUNK)].T

        return carry

    lax.fori_loop(0, 8, finish, 0)

    for d in range(1, 4):
        stats_copy(d).wait_send()
    for c in range(4):

        @pl.when(has_prev & ((x < 3) | (c < 2)))
        def _():
            back_copy(c).wait_send()

        for k in (1, 3):
            ring_copy(k, 0, c).wait_send()

            @pl.when(relays(k, c))
            def _():
                relay_copy(k, c).wait_send()


    @pl.when(has_prev)
    def _():
        affine_back().wait_send()

    for k in (1, 3):
        affine_ring(k, 0).wait_send()

        @pl.when(relays_affine(k))
        def _():
            affine_relay(k).wait_send()


    def drain_core(v, carry):
        t, hm = v // 8, v % 8
        h, m = hm // 4, hm % 4
        core_copy((2 * t + h) * 4 + m).wait_send()
        return carry

    lax.fori_loop(0, 16, drain_core, 0)

    def drain(v, carry):
        @pl.when(sends_mirror & (v % 4 == 0))
        def _():
            upper_copy(v).wait_send()

        @pl.when(jnp.logical_not(sends_mirror & (v % 4 == 0)))
        def _():
            cross_copy(v).wait_send()

        return carry

    lax.fori_loop(0, 8, drain, 0)


def on_device(genotypes):
    samples, snps = genotypes.shape
    dma = pltpu.SemaphoreType.DMA
    return pl.pallas_call(
        kernel,
        out_shape=jax.ShapeDtypeStruct((snps, BAND // lax.axis_size("samp")), jnp.float32),
        in_specs=[pl.BlockSpec(memory_space=pltpu.HBM)],
        out_specs=pl.BlockSpec(memory_space=pltpu.VMEM),
        scratch_shapes=[
            pltpu.VMEM((4, samples, CHUNK), jnp.float32),
            pltpu.VMEM((4, 8, snps), jnp.float32),
            pltpu.VMEM((20, samples, CHUNK), jnp.bfloat16),
            pltpu.VMEM((5, 2, snps), jnp.float32),
            pltpu.VMEM((4, samples, CHUNK), jnp.bfloat16),
            pltpu.VMEM((samples, CHUNK), jnp.bfloat16),
            pltpu.VMEM((snps, samples), jnp.bfloat16),
            pltpu.VMEM((16, TILE, CHUNK), jnp.float32),
            pltpu.VMEM((16, TILE, CHUNK), jnp.bfloat16),
            pltpu.VMEM((16, TILE, CHUNK), jnp.bfloat16),
            pltpu.VMEM((8, TILE, CHUNK), jnp.bfloat16),
            pltpu.VMEM((8, TILE, CHUNK), jnp.bfloat16),
            dma((4,)),
            dma((3,)),
            dma((4,)),
            dma((4,)),
            dma((3, 4)),
            dma((8,)),
            dma((20,)),
            dma((6,)),
            dma((5,)),
            dma((16,)),
            dma((16,)),
            dma((8,)),
            dma((8,)),
        ],
        compiler_params=pltpu.CompilerParams(
            collective_id=0, has_side_effects=True, vmem_limit_bytes=47 * 2**20
        ),
        name="ld_band",
    )(genotypes)


def solution(mesh):
    return jax.shard_map(
        on_device, mesh=mesh, in_specs=(P("samp", "snp"),), out_specs=P("snp", "samp"), check_vma=False
    )
```
